128 devices in a mesh: rows: 32 (over z, y, core), cols: 4 (over x).
Axes of the slice: x: 4, y: 4, z: 4, core: 2. Of those that a mesh axis runs over, the one named last changes fastest.
Arguments:
- w_gate: float32 [2048, 8192], P('rows', 'cols'), may hold values from -0.25 to 0.25
- first_gate: float32 [2048, 8192], P('rows', 'cols'), may hold values from -6 to 6
- second_gate: float32 [2048, 8192], P('rows', 'cols'), may hold values from 0.1 to 10
- w_up: float32 [2048, 8192], P('rows', 'cols'), may hold values from -0.25 to 0.25
- first_up: float32 [2048, 8192], P('rows', 'cols'), may hold values from -6 to 6
- second_up: float32 [2048, 8192], P('rows', 'cols'), may hold values from 0.1 to 10
- norm_train: float32 [2048], P(('rows', 'cols')), may hold values from 0.25 to 1.75
- norm_step: float32 [2048], P(('rows', 'cols')), may hold values from -0.3 to 0.3
Outputs:
- ready_gate: bfloat16 [2048, 8192], P(None, 'cols')
- ready_up: bfloat16 [2048, 8192], P(None, 'cols')
- column_gate: float32 [8192], P('cols')
- column_up: float32 [8192], P('cols')
- serve_norm: bfloat16 [2048], replicated
- latest_gate: float32 [2048, 8192], P('rows', 'cols')
- latest_up: float32 [2048, 8192], P('rows', 'cols')
The draws below stay inside these ranges and needn't reach their ends.
All inputs are finite; a program needn't handle non-finite values. Where the reference program divides by a largest or mean magnitude, that divisor is 1e-20 or more.
Results may differ from the reference program's by a relative error of at most 0.001.
Values may be sent and summed in bfloat16 or wider, within the bound.
No kernel may reach another device: no remote copies, remote signals or barrier semaphores. Data moves between devices by JAX's collectives and lax.ppermute only.
A program may use at most 128 MiB of HBM per device.

```python
import math
import jax
import jax.numpy as jnp
from jax import lax

D_MODEL = 2048
D_INNER = 8192


def raised(result, key, source, target, parts, factor):
    def block_of(axis_at):
        return (jnp.arange(result.shape[axis_at]) // (result.shape[axis_at] // parts)).reshape((-1,) + (1,) * (result.ndim - 1 - axis_at))

    one_side = jax.random.permutation(key, parts)[block_of(target)]
    other_side = (block_of(target) + parts // 2) % parts
    return jnp.where((block_of(source) == one_side) | (block_of(source) == other_side), factor * result, result)


def levels(key, extent, shards, low, top_value):
    factor_of, own = 1.0, jax.random.fold_in(key, 6)
    for position, shards_of in shards:
        heights = jnp.exp(jax.random.uniform(jax.random.fold_in(own, position), (shards_of,), jnp.float32, low / len(shards), top_value / len(shards)))
        factor_of = factor_of * jnp.repeat(heights, extent[position] // shards_of).reshape([-1 if axis == position else 1 for axis in range(len(extent))])
    return factor_of


def noise(stream_key, dims, scale, bound, cuts=(), held_as=jnp.bfloat16):
    entries = jax.random.normal(stream_key, dims, jnp.float32) * scale
    if len(cuts) > 0:
        entries = levels(stream_key, dims, cuts, -0.22, 0.18) * entries
    return jnp.clip(entries, min=-bound, max=bound).astype(held_as)


def gaussian_with(rng, dims, width, limit, pieces, heavy, kind=jnp.bfloat16):
    entries = width * jax.random.normal(rng, dims, jnp.float32)
    if pieces:
        entries = entries * levels(rng, dims, pieces, -0.22, 0.18)
    return jnp.clip(raised(entries, jax.random.fold_in(rng, 3), *heavy), -limit, limit).astype(kind)


def setup_inputs(seed: int = 0) -> dict:
    streams_of = jax.random.split(jax.random.key(seed), 9)
    w_gate = gaussian_with(streams_of[0], (D_MODEL, D_INNER), D_MODEL ** -0.5, 0.25, ((0, 32), (1, 4)), (0, 1, 32, 2.75), jnp.float32)
    first_gate = noise(streams_of[1], (D_MODEL, D_INNER), 1.0, 6.0, ((0, 32), (1, 4)), jnp.float32)
    second_gate = jnp.clip(jnp.exp(math.log(10.0) - 4.6051702 * jax.random.uniform(streams_of[2], (D_MODEL, D_INNER), jnp.float32) ** levels(streams_of[2], (D_MODEL, D_INNER), ((0, 32), (1, 4)), -0.2, 0.2)), 0.1, 10.0)
    w_up = gaussian_with(streams_of[3], (D_MODEL, D_INNER), D_MODEL ** -0.5, 0.25, ((0, 32), (1, 4)), (0, 1, 32, 2.75), jnp.float32)
    first_up = noise(streams_of[4], (D_MODEL, D_INNER), 1.0, 6.0, ((0, 32), (1, 4)), jnp.float32)
    second_up = jnp.clip(jnp.exp(math.log(10.0) - 4.6051702 * jax.random.uniform(streams_of[5], (D_MODEL, D_INNER), jnp.float32) ** levels(streams_of[5], (D_MODEL, D_INNER), ((0, 32), (1, 4)), -0.2, 0.2)), 0.1, 10.0)
    norm_train = jnp.clip(1.0 + 0.15 * jax.random.normal(streams_of[6], (D_MODEL,), jnp.float32), 0.25, 1.75)
    norm_step = jnp.clip(jax.random.uniform(streams_of[7], (D_MODEL,), jnp.float32, -0.3, 0.3) * levels(streams_of[7], (D_MODEL,), ((0, 128),), -0.4, 0.0), -0.3, 0.3)
    return dict(w_gate=w_gate, first_gate=first_gate, second_gate=second_gate, w_up=w_up, first_up=first_up, second_up=second_up, norm_train=norm_train, norm_step=norm_step)


learn_rate = 0.01
decay_rate = 0.1
tiny_value = 1e-08

def reference(w_gate, first_gate, second_gate, w_up, first_up, second_up, norm_train, norm_step):
    latest_gate = w_gate - learn_rate * (first_gate / (jnp.sqrt(second_gate) + tiny_value) + decay_rate * w_gate)
    latest_up = w_up - learn_rate * (first_up / (jnp.sqrt(second_up) + tiny_value) + decay_rate * w_up)
    column_gate = lax.optimization_barrier(jnp.sum(jnp.abs(latest_gate), axis=0)) / D_MODEL
    ready_gate = (latest_gate / column_gate).astype(jnp.bfloat16)
    column_up = lax.optimization_barrier(jnp.sum(jnp.abs(latest_up), axis=0)) / D_MODEL
    ready_up = (latest_up / column_up).astype(jnp.bfloat16)
    serve_norm = (norm_train + norm_step).astype(jnp.bfloat16)
    return (ready_gate, ready_up, column_gate, column_up, serve_norm, latest_gate, latest_up)
```

```python
import functools
import jax
import jax.numpy as jnp
from jax import lax
from jax.experimental import pallas as pl
from jax.experimental.pallas import tpu as pltpu
from jax.sharding import Mesh
from jax.sharding import PartitionSpec as P

D_MODEL = 2048
ROWS = ("z", "y", "core")
ALL = ("z", "y", "core", "x")

learn_rate = 0.01
decay_rate = 0.1
tiny_value = 1e-08

OCTAVES = 252.0
LOWEST = -125.0
SLABS = 16
BLOCK = 64 * SLABS + SLABS
VMEM = pl.BlockSpec(memory_space=pltpu.VMEM)
HBM = pl.BlockSpec(memory_space=pltpu.HBM)
SMALL = pltpu.CompilerParams(vmem_limit_bytes=4 << 20)


def number(z, y, c):
    return (z % 4 * 4 + y % 4) * 2 + c


def near_far(by_near, by_far):
    return [
        (number(z, y, c), number(z + by_far, y + by_near, c) if c == 0 else number(z + by_near, y + by_far, c))
        for z in range(4)
        for y in range(4)
        for c in range(2)
    ]


def near(value, by):
    return lax.ppermute(value, ROWS, near_far(by, 0))


def far(value, by):
    return lax.ppermute(value, ROWS, near_far(0, by))


def swapped(value):
    return lax.ppermute(value, "core", [(0, 1), (1, 0)])


def step_kernel(w_g, f_g, s_g, w_u, f_u, s_u, latest_g, latest_u, code, sums, *scratch):
    held, sem = scratch[:6], scratch[6]
    wide = 512
    chunks = D_MODEL // wide
    sources = (w_g, f_g, s_g, w_u, f_u, s_u)
    copies = []
    for k in range(chunks):
        at = pl.ds(k * wide, wide)
        for i in range(6):
            one = pltpu.make_async_copy(sources[i].at[:, at], held[i].at[:, at], sem.at[k * 6 + i])
            one.start()
            copies.append(one)
    for k in range(chunks):
        for o, latest in ((0, latest_g), (1, latest_u)):
            for i in range(3):
                copies[k * 6 + 3 * o + i].wait()
            for slab in range(k * wide // 128, (k + 1) * wide // 128):
                at = pl.ds(slab * 128, 128)
                w, first, second = (held[3 * o + i][:, at] for i in range(3))
                new = w - learn_rate * (first / (jnp.sqrt(second) + tiny_value) + decay_rate * w)
                latest[:, at] = new
                size = jnp.abs(new)
                sums[pl.ds(SLABS * o + slab, 1), :] = jnp.sum(size, axis=0, keepdims=True)
                top = (jnp.max(size, axis=0, keepdims=True) * 1.01).astype(jnp.bfloat16)
                scale = OCTAVES / jnp.maximum(top.astype(jnp.float32), 1e-35)
                value = jnp.exp2(size * scale + LOWEST)
                code[pl.ds(BLOCK * o + 64 * slab, 64), :] = jnp.where(new < 0, -value, value).astype(jnp.bfloat16)
                scratch[7][pl.ds(SLABS * o + slab, 1), :] = top.astype(jnp.float32)
    for o in (0, 1):
        code[pl.ds(BLOCK * o + 64 * SLABS, SLABS), :] = scratch[7][pl.ds(SLABS * o, SLABS), :].astype(jnp.bfloat16)


def stepped(*arrays):
    weights = jax.ShapeDtypeStruct((64, D_MODEL), jnp.float32)
    return pl.pallas_call(
        step_kernel,
        out_shape=(
            weights,
            weights,
            jax.ShapeDtypeStruct((2 * BLOCK, 128), jnp.bfloat16),
            jax.ShapeDtypeStruct((2 * SLABS, 128), jnp.float32),
        ),
        in_specs=[HBM] * 6,
        out_specs=(VMEM,) * 4,
        scratch_shapes=[pltpu.VMEM((64, D_MODEL), jnp.float32)] * 6
        + [pltpu.SemaphoreType.DMA((24,)), pltpu.VMEM((2 * SLABS, 128), jnp.float32)],
        compiler_params=pltpu.CompilerParams(vmem_limit_bytes=8 << 20),
        name="step",
    )(*arrays)


def pack_kernel(spans, *refs):
    out, at = refs[-1], 0
    for ref, (lo, n) in zip(refs, spans):
        for k in range(0, n, 208):
            out[pl.ds(at + k, 208), :] = ref[pl.ds(lo + k, 208), :]
        at += n


def packed(*parts):
    spans = tuple((lo * BLOCK, n * BLOCK) for _, lo, n in parts)
    return pl.pallas_call(
        functools.partial(pack_kernel, spans),
        out_shape=jax.ShapeDtypeStruct((sum(n for _, n in spans), 128), jnp.bfloat16),
        in_specs=[VMEM] * len(parts),
        out_specs=VMEM,
        compiler_params=SMALL,
        name="pack",
    )(*(a for a, _, _ in parts))


def home(core_away, a, b):
    z, y, c = (lax.axis_index(axis) for axis in ROWS)
    c = lax.rem(c + core_away, 2)
    dz, dy = a + (b - a) * (1 - c), b + (a - b) * (1 - c)
    at = (lax.rem(z + 4 - dz, 4) * 4 + lax.rem(y + 4 - dy, 4)) * 2 + c
    return pl.ds(pl.multiple_of(at * 64, 64), 64)


def decode_kernel(plan, write, n, *refs):
    arrays, total = refs[:n], refs[n]
    plain, factor = (refs[-5], refs[-1]) if write else (refs[-2], refs[-1])
    outs, sem = (refs[-4:-2], refs[-2]) if write else (None, None)
    copies = []
    for k, (i, at, o, a, b) in enumerate(plan):
        ref = arrays[i]
        inverse = (D_MODEL / OCTAVES) / total[pl.ds(SLABS * o, SLABS), :]
        factor[...] = ref[pl.ds(at * BLOCK + 64 * SLABS, SLABS), :].astype(jnp.float32) * inverse

        def slab(j, carry, ref=ref, at=at, k=k):
            rows = pl.ds(pl.multiple_of(at * BLOCK + j * 64, 16), 64)
            value = ref[rows, :].astype(jnp.float32)
            size = (jnp.log2(jnp.abs(value)) - LOWEST) * factor[pl.ds(j, 1), :]
            plain[pl.ds(64 * k, 64), pl.ds(pl.multiple_of(j * 128, 128), 128)] = jnp.where(
                value < 0, -size, size
            ).astype(jnp.bfloat16)
            return carry

        lax.fori_loop(0, SLABS, slab, 0, unroll=2)
        if write:
            one = pltpu.make_async_copy(plain.at[pl.ds(64 * k, 64), :], outs[o].at[home(0, a, b), :], sem.at[k])
            one.start()
            copies.append(one)
    for one in copies:
        one.wait()


READY = jax.ShapeDtypeStruct((D_MODEL, D_MODEL), jnp.bfloat16)


def decoded(outs, arrays, plan, total, write=True):
    n, fresh = len(arrays), outs is None
    plain = jax.ShapeDtypeStruct((64 * len(plan), D_MODEL), jnp.bfloat16)
    got = pl.pallas_call(
        functools.partial(decode_kernel, plan, write, n),
        out_shape=(plain, READY, READY) if write else plain,
        in_specs=[VMEM] * (n + 1) + ([HBM] * 2 if write and not fresh else []),
        out_specs=(VMEM, HBM, HBM) if write else VMEM,
        scratch_shapes=([pltpu.SemaphoreType.DMA((len(plan),))] if write else [])
        + [pltpu.VMEM((SLABS, 128), jnp.float32)],
        input_output_aliases={n + 1: 1, n + 2: 2} if write and not fresh else {},
        compiler_params=SMALL,
    )(*arrays, total, *(outs if write and not fresh else ()))
    return (got[0], got[1:]) if write else (got, outs)


def write_kernel(plan, *refs):
    n = len(plan)
    arrays, outs, sem = refs[:n], refs[-3:-1], refs[-1]
    copies = []
    for ref, (core_away, blocks) in zip(arrays, plan):
        for k, (o, a, b) in enumerate(blocks):
            copies.append(
                pltpu.make_async_copy(
                    ref.at[pl.ds(64 * k, 64), :], outs[o].at[home(core_away, a, b), :], sem.at[len(copies)]
                )
            )
    for one in copies:
        one.start()
    for one in copies:
        one.wait()


def written(outs, batch):
    n = len(batch)
    plan = tuple((core_away, tuple(p[2:] for p in blocks)) for _, core_away, blocks in batch)
    return pl.pallas_call(
        functools.partial(write_kernel, plan),
        out_shape=(READY, READY),
        in_specs=[VMEM] * n + [HBM] * 2,
        out_specs=(HBM, HBM),
        scratch_shapes=[pltpu.SemaphoreType.DMA((sum(len(b) for _, b in plan),))],
        input_output_aliases={n: 0, n + 1: 1},
        compiler_params=SMALL,
    )(*(a for a, _, _ in batch), *outs)


def local(w_gate, first_gate, second_gate, w_up, first_up, second_up, norm_train, norm_step):
    latest_gate, latest_up, own, sums = stepped(w_gate, first_gate, second_gate, w_up, first_up, second_up)
    r, l = near(own, 1), near(own, 3)

    me = (lax.axis_index("z") * 4 + lax.axis_index("y")) * 2 + lax.axis_index("core")
    gain = (norm_train + norm_step).astype(jnp.bfloat16).astype(jnp.float32)
    spread = lax.dynamic_update_slice(
        jnp.zeros((128, 16), jnp.float32), gain[None], (me * 4 + lax.axis_index("x"), 0)
    )
    sums = jnp.concatenate((sums, spread.reshape(SLABS, 128)), axis=0)
    sums = sums + far(sums, 1) + far(sums, 3) + far(sums, 2)
    sums = sums + near(sums, 1) + near(sums, 3) + near(sums, 2)
    sums = sums + swapped(sums)
    column_gate = sums[:SLABS].reshape(D_MODEL) / D_MODEL
    column_up = sums[SLABS : 2 * SLABS].reshape(D_MODEL) / D_MODEL
    norm = sums[2 * SLABS :]
    for by in (1, 3, 2):
        other = lax.ppermute(sums[2 * SLABS :], "x", [(i, (i + by) % 4) for i in range(4)])
        norm = norm + other
    serve_norm = norm.reshape(D_MODEL).astype(jnp.bfloat16)
    total = sums[: 2 * SLABS]

    fa = {by: far(own, by) for by in (1, 3)}
    og, ou = near(packed((r, 0, 1)), 1), near(packed((l, 1, 1)), 3)
    rl = packed((r, 0, 1), (l, 0, 1), (r, 1, 1), (l, 1, 1))
    fb = {by: far(rl, by) for by in (1, 3)}
    o = packed((og, 0, 1), (ou, 0, 1))
    fc = {by: far(o, by) for by in (1, 3)}
    ga_g = far(packed((fa[1], 0, 1), (fb[1], 0, 2)), 1)
    ga_u = far(packed((fa[3], 1, 1), (fb[3], 2, 2)), 3)
    gb_g = far(packed((fc[1], 0, 1)), 1)
    gb_u = far(packed((fc[3], 1, 1)), 3)

    def pair(i, a, b):
        return [(i, 0, 0, a, b), (i, 1, 1, a, b)]

    def four(i, b):
        return [(i, 0, 0, 1, b), (i, 1, 0, 3, b), (i, 2, 1, 1, b), (i, 3, 1, 3, b)]

    batches = [
        ([own, rl, o, fa[1], fa[3]], pair(0, 0, 0) + four(1, 0) + pair(2, 2, 0) + pair(3, 0, 1) + pair(4, 0, 3)),
        ([fb[1], fb[3]], four(0, 1) + four(1, 3)),
        ([fc[1], fc[3]], pair(0, 2, 1) + pair(1, 2, 3)),
        ([ga_g, ga_u], [(o, i, o, a, 2) for o in (0, 1) for i, a in enumerate((0, 1, 3))]),
        ([gb_g, gb_u], [(o, 0, o, 2, 2) for o in (0, 1)]),
    ]
    outs = None
    for j, (arrays, plan) in enumerate(batches):
        last = j == len(batches) - 1
        plain, outs = decoded(outs, arrays, tuple(plan), total, write=not last)
        other = swapped(plain)
        outs = written(outs, ([(plain, 0, plan)] if last else []) + [(other, 1, plan)])
    return (outs[0], outs[1], column_gate, column_up, serve_norm, latest_gate, latest_up)


def solution(mesh):
    torus = Mesh(mesh.devices.reshape(4, 4, 2, mesh.shape["cols"]), ALL)
    whole = P(ROWS, "x")
    return jax.shard_map(
        local,
        mesh=torus,
        in_specs=(whole,) * 6 + (P(ALL),) * 2,
        out_specs=(P(None, "x"), P(None, "x"), P("x"), P("x"), P(), whole, whole),
        check_vma=False,
    )
```

```python
import functools
import math
import jax
import jax.numpy as jnp
from jax import lax
from jax.experimental import pallas as pl
from jax.experimental.pallas import tpu as pltpu
from jax.sharding import Mesh
from jax.sharding import PartitionSpec as P

D_MODEL = 2048
ROWS = ("z", "y", "core")
ALL = ("z", "y", "core", "x")

learn_rate = 0.01
decay_rate = 0.1
tiny_value = 1e-08

OCTAVES = 125.5
SLABS = 16
UNROLL = 16
BLOCK = 64 * SLABS + SLABS
VMEM = pl.BlockSpec(memory_space=pltpu.VMEM)
HBM = pl.BlockSpec(memory_space=pltpu.HBM)
READY = jax.ShapeDtypeStruct((D_MODEL, D_MODEL), jnp.bfloat16)

DECODES = {
    "dec_0": (("a", 0), ("a", 1)),
    "dec_1": (("b", 0), ("b", 1)),
    "dec_2": (("c", 0), ("c", 1)),
    "dec_3": (("g1", 0),),
    "dec_4": (("g1", 1), ("g2", 0)),
    "dec_5": (("g2", 1),),
}
HELD = {
    "a": [(o, a, 0) for o in (0, 1) for a in (0, 1, 3)],
    "b": [(o, 0, b) for b in (1, 3) for o in (0, 1)] + [(o, a, b) for b in (1, 3) for o in (0, 1) for a in (1, 3)],
    "c": [(o, 2, b) for b in (0, 1, 3) for o in (0, 1)],
    "g1": [(o, a, 2) for o in (0, 1) for a in (0, 1, 3)],
    "g2": [(o, 2, 2) for o in (0, 1)],
}


def number(z, y, c):
    return (z % 4 * 4 + y % 4) * 2 + c


def near_far(by_near, by_far):
    return [
        (number(z, y, c), number(z + by_far, y + by_near, c) if c == 0 else number(z + by_near, y + by_far, c))
        for z in range(4)
        for y in range(4)
        for c in range(2)
    ]


def near(value, by):
    return lax.ppermute(value, ROWS, near_far(by, 0))


def far(value, by):
    return lax.ppermute(value, ROWS, near_far(0, by))


def swapped(value):
    return lax.ppermute(value, "core", [(0, 1), (1, 0)])


def step_kernel(w_g, f_g, s_g, w_u, f_u, s_u, norm, change, latest_g, latest_u, code, sums, *scratch):
    held, sem, tops, gains = scratch[:6], scratch[6], scratch[7], scratch[8]
    wide = 512
    chunks = D_MODEL // wide
    sources = (w_g, f_g, s_g, w_u, f_u, s_u)
    copies = []
    for k in range(chunks):
        at = pl.ds(k * wide, wide)
        for i in range(6):
            copies.append(pltpu.make_async_copy(sources[i].at[:, at], held[i].at[:, at], sem.at[k * 6 + i]))
    for i, source in enumerate((norm, change)):
        copies.append(pltpu.make_async_copy(source, gains.at[pl.ds(i, 1), :], sem.at[6 * chunks + i]))
    for one in copies:
        one.start()
    for k in range(chunks):
        for o, latest in ((0, latest_g), (1, latest_u)):
            for i in range(3):
                copies[k * 6 + 3 * o + i].wait()
            for slab in range(k * wide // 128, (k + 1) * wide // 128):
                at = pl.ds(slab * 128, 128)
                w, first, second = (held[3 * o + i][:, at] for i in range(3))
                new = w - learn_rate * (first / (jnp.sqrt(second) + tiny_value) + decay_rate * w)
                latest[:, at] = new
                size = jnp.abs(new)
                sums[pl.ds(SLABS * o + slab, 1), :] = jnp.sum(size, axis=0, keepdims=True)
                top = (jnp.max(size, axis=0, keepdims=True) * 1.01).astype(jnp.bfloat16).astype(jnp.float32)
                code[pl.ds(BLOCK * o + 64 * slab, 64), :] = jnp.exp2(new * (OCTAVES / jnp.maximum(top, 1e-35))).astype(
                    jnp.bfloat16
                )
                tops[pl.ds(SLABS * o + slab, 1), :] = top
    for o in (0, 1):
        code[pl.ds(BLOCK * o + 64 * SLABS, SLABS), :] = tops[pl.ds(SLABS * o, SLABS), :].astype(jnp.bfloat16)
    for one in copies[-2:]:
        one.wait()
    gain = (gains[pl.ds(0, 1), :] + gains[pl.ds(1, 1), :]).astype(jnp.bfloat16).astype(jnp.float32)
    gain = jnp.concatenate([gain] * 8, axis=1)
    me = (lax.axis_index("z") * 4 + lax.axis_index("y")) * 2 + lax.axis_index("core")
    place = me * 4 + lax.axis_index("x")
    row = lax.broadcasted_iota(jnp.int32, (SLABS, 128), 0)
    lane = lax.broadcasted_iota(jnp.int32, (SLABS, 128), 1)
    sums[pl.ds(2 * SLABS, SLABS), :] = jnp.where(row * 8 + lane // 16 == place, gain, 0.0)


def stepped(*arrays):
    weights = pltpu.VMEM((64, D_MODEL), jnp.float32)
    return pl.pallas_call(
        step_kernel,
        out_shape=(
            weights,
            weights,
            jax.ShapeDtypeStruct((2 * BLOCK, 128), jnp.bfloat16),
            jax.ShapeDtypeStruct((3 * SLABS, 128), jnp.float32),
        ),
        in_specs=[HBM] * 8,
        out_specs=(VMEM,) * 4,
        scratch_shapes=[pltpu.VMEM((64, D_MODEL), jnp.float32)] * 6
        + [pltpu.SemaphoreType.DMA((26,)), pltpu.VMEM((2 * SLABS, 128), jnp.float32), pltpu.VMEM((2, 16), jnp.float32)],
        compiler_params=pltpu.CompilerParams(vmem_limit_bytes=8 << 20),
        name="step",
    )(*(pltpu.with_memory_space_constraint(a, pltpu.HBM) for a in arrays))


def pack_kernel(spans, *refs):
    out, at = refs[-1], 0
    for ref, (lo, n) in zip(refs, spans):
        for k in range(0, n, 208):
            out[pl.ds(at + k, 208), :] = ref[pl.ds(lo + k, 208), :]
        at += n


def packed(*parts):
    spans = tuple((lo * BLOCK, n * BLOCK) for _, lo, n in parts)
    return pl.pallas_call(
        functools.partial(pack_kernel, spans),
        out_shape=jax.ShapeDtypeStruct((sum(n for _, n in spans), 128), jnp.bfloat16),
        in_specs=[VMEM] * len(parts),
        out_specs=VMEM,
        compiler_params=pltpu.CompilerParams(vmem_limit_bytes=2 << 20),
        name="pack",
    )(*(a for a, _, _ in parts))


def home(core_away, a, b):
    z, y, c = (lax.axis_index(axis) for axis in ROWS)
    c = lax.rem(c + core_away, 2)
    dz, dy = a + (b - a) * (1 - c), b + (a - b) * (1 - c)
    at = (lax.rem(z + 4 - dz, 4) * 4 + lax.rem(y + 4 - dy, 4)) * 2 + c
    return pl.ds(pl.multiple_of(at * 64, 64), 64)


def decode_kernel(plan, n, n_kept, n_out, *refs):
    arrays, total, extra = refs[:n], refs[n], refs[n + 1 : n + 1 + n_kept]
    plain, factor, sem = refs[-3:]
    got = refs[len(refs) - 3 - n_out : -3]
    outs, kept = got[:2], got[2:]
    blocks = [(ref, k, away, block) for ref, (name, away) in zip(arrays, plan) for k, block in enumerate(HELD[name])]
    copies = [pltpu.make_async_copy(a, b, sem.at[len(blocks) + i]) for i, (a, b) in enumerate(zip(extra, kept))]
    for one in copies:
        one.start()
    for n, (ref, k, away, (o, a, b)) in enumerate(blocks):
        factor[...] = ref[pl.ds(k * BLOCK + 64 * SLABS, SLABS), :].astype(jnp.float32) * (
            (D_MODEL / OCTAVES / math.log(2.0)) / total[pl.ds(SLABS * o, SLABS), :]
        )

        def slab(j, carry, ref=ref, at=k * BLOCK, to=64 * n):
            rows = pl.ds(pl.multiple_of(at + j * 64, 16), 64)
            value = jnp.log(ref[rows, :].astype(jnp.float32)) * factor[pl.ds(j, 1), :]
            plain[pl.ds(to, 64), pl.ds(pl.multiple_of(j * 128, 128), 128)] = value.astype(jnp.bfloat16)
            return carry

        lax.fori_loop(0, SLABS, slab, 0, unroll=UNROLL)
        one = pltpu.make_async_copy(plain.at[pl.ds(64 * n, 64), :], outs[o].at[home(away, a, b), :], sem.at[n])
        one.start()
        copies.append(one)
    for one in copies:
        one.wait()


def decoded(outs, arrays, plan, total, extra=()):
    n, aliased = len(arrays), 2 * (outs is not None)
    blocks = sum(len(HELD[name]) for name, _ in plan)
    out_shape = (READY, READY) + tuple(jax.ShapeDtypeStruct(a.shape, a.dtype) for a in extra)
    got = pl.pallas_call(
        functools.partial(decode_kernel, plan, n, len(extra), len(out_shape)),
        out_shape=out_shape,
        in_specs=[VMEM] * (n + 1 + len(extra)) + [HBM] * aliased,
        out_specs=(HBM,) * len(out_shape),
        scratch_shapes=[
            pltpu.VMEM((64 * blocks, D_MODEL), jnp.bfloat16),
            pltpu.VMEM((SLABS, 128), jnp.float32),
            pltpu.SemaphoreType.DMA((blocks + len(extra),)),
        ],
        input_output_aliases={n + 1 + len(extra) + i: i for i in range(aliased)},
        compiler_params=pltpu.CompilerParams(vmem_limit_bytes=(1 << 20) + 64 * blocks * D_MODEL * 2),
    )(*arrays, total, *extra, *(outs if aliased else ()))
    return got[:2], got[2:]


def local(w_gate, first_gate, second_gate, w_up, first_up, second_up, norm_train, norm_step):
    latest_gate, latest_up, own, sums = stepped(
        w_gate, first_gate, second_gate, w_up, first_up, second_up, norm_train[None], norm_step[None]
    )
    r, l = near(own, 1), near(own, 3)
    o = packed((near(packed((r, 0, 1)), 1), 0, 1), (near(packed((l, 1, 1)), 3), 0, 1))
    sums = sums + far(sums, 1) + far(sums, 3) + far(sums, 2)
    norm = sums[2 * SLABS :]
    for to in ((1, 0, 3, 2), (3, 2, 1, 0)):
        other = lax.ppermute(norm, "x", list(enumerate(to)))
        norm = norm + other
    sums = jnp.concatenate((sums[: 2 * SLABS], norm), axis=0)
    sums = sums + near(sums, 1) + near(sums, 3) + near(sums, 2)
    sums = sums + swapped(sums)
    total = sums[: 2 * SLABS]
    column_gate = total[:SLABS].reshape(D_MODEL) / D_MODEL
    column_up = total[SLABS:].reshape(D_MODEL) / D_MODEL
    serve_norm = sums[2 * SLABS :].reshape(D_MODEL).astype(jnp.bfloat16)

    first = packed(*((a, at, 1) for at in (0, 1) for a in (r, l)))
    got = {}
    for by in (1, 3):
        for name, value in (("fa", own), ("f1", first), ("f2", o)):
            got[name, by] = far(value, by)
    halves = ((0, 1), (1, 3))
    g1 = [far(packed((got["fa", by], half, 1), (got["f1", by], 2 * half, 2)), by) for half, by in halves]
    g2 = [far(packed((got["f2", by], half, 1)), by) for half, by in halves]
    mine = {
        "a": packed(*((a, at, 1) for at in (0, 1) for a in (own, r, l))),
        "b": packed(*((got["fa", by], 0, 2) for by in (1, 3)), *((got["f1", by], 0, 4) for by in (1, 3))),
        "c": packed((o, 0, 2), *((got["f2", by], 0, 2) for by in (1, 3))),
        "g1": packed(*((a, 0, 3) for a in g1)),
        "g2": packed(*((a, 0, 1) for a in g2)),
    }
    held = (mine, {name: swapped(value) for name, value in mine.items()})
    outs = None
    for label, plan in DECODES.items():
        extra = {"dec_0": (latest_gate, latest_up), "dec_1": (column_gate, column_up), "dec_3": (serve_norm,)}.get(label, ())
        outs, kept = decoded(outs, [held[away][name] for name, away in plan], plan, total, extra)
        if label == "dec_0":
            latest_gate, latest_up = kept
        if label == "dec_1":
            column_gate, column_up = kept
        if label == "dec_3":
            (serve_norm,) = kept
    return (outs[0], outs[1], column_gate, column_up, serve_norm, latest_gate, latest_up)


def solution(mesh):
    torus = Mesh(mesh.devices.reshape(4, 4, 2, mesh.shape["cols"]), ALL)
    whole = P(ROWS, "x")
    return jax.shard_map(
        local,
        mesh=torus,
        in_specs=(whole,) * 6 + (P(ALL),) * 2,
        out_specs=(P(None, "x"), P(None, "x"), P("x"), P("x"), P(), whole, whole),
        check_vma=False,
    )
```

```python
import functools
import math
import jax
import jax.numpy as jnp
from jax import lax
from jax.experimental import pallas as pl
from jax.experimental.pallas import tpu as pltpu
from jax.sharding import Mesh
from jax.sharding import PartitionSpec as P

D_MODEL = 2048
ROWS = ("z", "y", "core")
ALL = ("z", "y", "core", "x")

learn_rate = 0.01
decay_rate = 0.1
tiny_value = 1e-08

OCTAVES = 125.5
SLABS = 16
UNROLL = 16
BLOCK = 64 * SLABS + SLABS
VMEM = pl.BlockSpec(memory_space=pltpu.VMEM)
HBM = pl.BlockSpec(memory_space=pltpu.HBM)
READY = jax.ShapeDtypeStruct((D_MODEL, D_MODEL), jnp.bfloat16)

DECODES = {
    "dec_0": (("a", 0), ("a", 1)),
    "dec_1": (("b", 0), ("b", 1)),
    "dec_2": (("c", 0), ("c", 1)),
    "dec_3": (("g1a", 0), ("g1b", 0)),
    "dec_4": (("g1a", 1), ("g1b", 1), ("g2", 0)),
    "dec_5": (("g2", 1),),
}
HELD = {
    "a": [(o, a, 0) for o in (0, 1) for a in (0, 1, 3)],
    "b": [(o, 0, b) for b in (1, 3) for o in (0, 1)] + [(o, a, b) for b in (1, 3) for o in (0, 1) for a in (1, 3)],
    "c": [(o, 2, b) for b in (0, 1, 3) for o in (0, 1)],
    "g1a": [(0, a, 2) for a in (0, 1, 3)],
    "g1b": [(1, a, 2) for a in (0, 1, 3)],
    "g2": [(o, 2, 2) for o in (0, 1)],
}


def number(z, y, c):
    return (z % 4 * 4 + y % 4) * 2 + c


def near_far(by_near, by_far):
    return [
        (number(z, y, c), number(z + by_far, y + by_near, c) if c == 0 else number(z + by_near, y + by_far, c))
        for z in range(4)
        for y in range(4)
        for c in range(2)
    ]


def near(value, by):
    return lax.ppermute(value, ROWS, near_far(by, 0))


def far(value, by):
    return lax.ppermute(value, ROWS, near_far(0, by))


def swapped(value):
    return lax.ppermute(value, "core", [(0, 1), (1, 0)])


def step_kernel(w_g, f_g, s_g, w_u, f_u, s_u, norm, change, latest_g, latest_u, code, sums, *scratch):
    held, sem, tops, gains = scratch[:6], scratch[6], scratch[7], scratch[8]
    wide = 1024
    chunks = D_MODEL // wide
    sources = (w_g, f_g, s_g, w_u, f_u, s_u)
    copies = []
    for k in range(chunks):
        at = pl.ds(k * wide, wide)
        for i in range(6):
            copies.append(pltpu.make_async_copy(sources[i].at[:, at], held[i].at[:, at], sem.at[k * 6 + i]))
    for i, source in enumerate((norm, change)):
        copies.append(pltpu.make_async_copy(source, gains.at[pl.ds(i, 1), :], sem.at[6 * chunks + i]))
    for one in copies:
        one.start()
    for k in range(chunks):
        for o, latest in ((0, latest_g), (1, latest_u)):
            for i in range(3):
                copies[k * 6 + 3 * o + i].wait()
            for slab in range(k * wide // 128, (k + 1) * wide // 128):
                at = pl.ds(slab * 128, 128)
                w, first, second = (held[3 * o + i][:, at] for i in range(3))
                new = w - learn_rate * (first / (jnp.sqrt(second) + tiny_value) + decay_rate * w)
                latest[:, at] = new
                size = jnp.abs(new)
                sums[pl.ds(SLABS * o + slab, 1), :] = jnp.sum(size, axis=0, keepdims=True)
                top = (jnp.max(size, axis=0, keepdims=True) * 1.01).astype(jnp.bfloat16).astype(jnp.float32)
                code[pl.ds(BLOCK * o + 64 * slab, 64), :] = jnp.exp2(new * (OCTAVES / jnp.maximum(top, 1e-35))).astype(
                    jnp.bfloat16
                )
                tops[pl.ds(SLABS * o + slab, 1), :] = top
    for o in (0, 1):
        code[pl.ds(BLOCK * o + 64 * SLABS, SLABS), :] = tops[pl.ds(SLABS * o, SLABS), :].astype(jnp.bfloat16)
    for one in copies[-2:]:
        one.wait()
    gain = (gains[pl.ds(0, 1), :] + gains[pl.ds(1, 1), :]).astype(jnp.bfloat16).astype(jnp.float32)
    gain = jnp.concatenate([gain] * 8, axis=1)
    me = (lax.axis_index("z") * 4 + lax.axis_index("y")) * 2 + lax.axis_index("core")
    place = me * 4 + lax.axis_index("x")
    row = lax.broadcasted_iota(jnp.int32, (SLABS, 128), 0)
    lane = lax.broadcasted_iota(jnp.int32, (SLABS, 128), 1)
    sums[pl.ds(2 * SLABS, SLABS), :] = jnp.where(row * 8 + lane // 16 == place, gain, 0.0)


def stepped(*arrays):
    weights = pltpu.VMEM((64, D_MODEL), jnp.float32)
    return pl.pallas_call(
        step_kernel,
        out_shape=(
            weights,
            weights,
            jax.ShapeDtypeStruct((2 * BLOCK, 128), jnp.bfloat16),
            jax.ShapeDtypeStruct((3 * SLABS, 128), jnp.float32),
        ),
        in_specs=[HBM] * 8,
        out_specs=(VMEM,) * 4,
        scratch_shapes=[pltpu.VMEM((64, D_MODEL), jnp.float32)] * 6
        + [pltpu.SemaphoreType.DMA((14,)), pltpu.VMEM((2 * SLABS, 128), jnp.float32), pltpu.VMEM((2, 16), jnp.float32)],
        compiler_params=pltpu.CompilerParams(vmem_limit_bytes=8 << 20),
        name="step",
    )(*(pltpu.with_memory_space_constraint(a, pltpu.HBM) for a in arrays))


def pack_kernel(spans, *refs):
    out, at = refs[-1], 0
    for ref, (lo, n) in zip(refs, spans):
        for k in range(0, n, 208):
            out[pl.ds(at + k, 208), :] = ref[pl.ds(lo + k, 208), :]
        at += n


def packed(*parts):
    spans = tuple((lo * BLOCK, n * BLOCK) for _, lo, n in parts)
    return pl.pallas_call(
        functools.partial(pack_kernel, spans),
        out_shape=jax.ShapeDtypeStruct((sum(n for _, n in spans), 128), jnp.bfloat16),
        in_specs=[VMEM] * len(parts),
        out_specs=VMEM,
        compiler_params=pltpu.CompilerParams(vmem_limit_bytes=2 << 20),
        name="pack",
    )(*(a for a, _, _ in parts))


def home(core_away, a, b):
    z, y, c = (lax.axis_index(axis) for axis in ROWS)
    c = lax.rem(c + core_away, 2)
    dz, dy = a + (b - a) * (1 - c), b + (a - b) * (1 - c)
    at = (lax.rem(z + 4 - dz, 4) * 4 + lax.rem(y + 4 - dy, 4)) * 2 + c
    return pl.ds(pl.multiple_of(at * 64, 64), 64)


def decode_kernel(plan, n, n_kept, n_out, *refs):
    arrays, total, extra = refs[:n], refs[n], refs[n + 1 : n + 1 + n_kept]
    plain, factor, sem = refs[-3:]
    got = refs[len(refs) - 3 - n_out : -3]
    outs, kept = got[:2], got[2:]
    blocks = [(ref, k, away, block) for ref, (name, away) in zip(arrays, plan) for k, block in enumerate(HELD[name])]
    copies = [pltpu.make_async_copy(a, b, sem.at[len(blocks) + i]) for i, (a, b) in enumerate(zip(extra, kept))]
    for one in copies:
        one.start()
    for n, (ref, k, away, (o, a, b)) in enumerate(blocks):
        factor[...] = ref[pl.ds(k * BLOCK + 64 * SLABS, SLABS), :].astype(jnp.float32) * (
            (D_MODEL / OCTAVES / math.log(2.0)) / total[pl.ds(SLABS * o, SLABS), :]
        )

        def slab(j, carry, ref=ref, at=k * BLOCK, to=64 * n):
            rows = pl.ds(pl.multiple_of(at + j * 64, 16), 64)
            value = jnp.log(ref[rows, :].astype(jnp.float32)) * factor[pl.ds(j, 1), :]
            plain[pl.ds(to, 64), pl.ds(pl.multiple_of(j * 128, 128), 128)] = value.astype(jnp.bfloat16)
            return carry

        lax.fori_loop(0, SLABS, slab, 0, unroll=UNROLL)
        one = pltpu.make_async_copy(plain.at[pl.ds(64 * n, 64), :], outs[o].at[home(away, a, b), :], sem.at[n])
        one.start()
        copies.append(one)
    for one in copies:
        one.wait()


def decoded(outs, arrays, plan, total, extra=()):
    n, aliased = len(arrays), 2 * (outs is not None)
    blocks = sum(len(HELD[name]) for name, _ in plan)
    out_shape = (READY, READY) + tuple(jax.ShapeDtypeStruct(a.shape, a.dtype) for a in extra)
    got = pl.pallas_call(
        functools.partial(decode_kernel, plan, n, len(extra), len(out_shape)),
        out_shape=out_shape,
        in_specs=[VMEM] * (n + 1 + len(extra)) + [HBM] * aliased,
        out_specs=(HBM,) * len(out_shape),
        scratch_shapes=[
            pltpu.VMEM((64 * blocks, D_MODEL), jnp.bfloat16),
            pltpu.VMEM((SLABS, 128), jnp.float32),
            pltpu.SemaphoreType.DMA((blocks + len(extra),)),
        ],
        input_output_aliases={n + 1 + len(extra) + i: i for i in range(aliased)},
        compiler_params=pltpu.CompilerParams(vmem_limit_bytes=(1 << 20) + 64 * blocks * D_MODEL * 2),
    )(*arrays, total, *extra, *(outs if aliased else ()))
    return got[:2], got[2:]


def local(w_gate, first_gate, second_gate, w_up, first_up, second_up, norm_train, norm_step):
    latest_gate, latest_up, own, sums = stepped(
        w_gate, first_gate, second_gate, w_up, first_up, second_up, norm_train[None], norm_step[None]
    )
    r, l = near(own, 1), near(own, 3)
    o = packed((near(packed((r, 0, 1)), 1), 0, 1), (near(packed((l, 1, 1)), 3), 0, 1))
    sums = sums + far(sums, 1) + far(sums, 3) + far(sums, 2)
    norm = sums[2 * SLABS :]
    for to in ((1, 0, 3, 2), (3, 2, 1, 0)):
        other = lax.ppermute(norm, "x", list(enumerate(to)))
        norm = norm + other
    sums = jnp.concatenate((sums[: 2 * SLABS], norm), axis=0)
    sums = sums + near(sums, 1) + near(sums, 3) + near(sums, 2)
    sums = sums + swapped(sums)
    total = sums[: 2 * SLABS]
    column_gate = total[:SLABS].reshape(D_MODEL) / D_MODEL
    column_up = total[SLABS:].reshape(D_MODEL) / D_MODEL
    serve_norm = sums[2 * SLABS :].reshape(D_MODEL).astype(jnp.bfloat16)

    first = packed(*((a, at, 1) for at in (0, 1) for a in (r, l)))
    got = {}
    for by in (1, 3):
        for name, value in (("fa", own), ("f1", first), ("f2", o)):
            got[name, by] = far(value, by)
    halves = ((0, 1), (1, 3))
    g1 = [far(packed((got["fa", by], half, 1), (got["f1", by], 2 * half, 2)), by) for half, by in halves]
    g2 = [far(packed((got["f2", by], half, 1)), by) for half, by in halves]
    mine = {
        "a": packed(*((a, at, 1) for at in (0, 1) for a in (own, r, l))),
        "b": packed(*((got["fa", by], 0, 2) for by in (1, 3)), *((got["f1", by], 0, 4) for by in (1, 3))),
        "c": packed((o, 0, 2), *((got["f2", by], 0, 2) for by in (1, 3))),
        "g1a": g1[0],
        "g1b": g1[1],
        "g2": packed(*((a, 0, 1) for a in g2)),
    }
    held = (mine, {name: swapped(value) for name, value in mine.items()})
    outs = None
    for label, plan in DECODES.items():
        extra = {"dec_0": (latest_gate, latest_up), "dec_1": (column_gate, column_up), "dec_3": (serve_norm,)}.get(label, ())
        outs, kept = decoded(outs, [held[away][name] for name, away in plan], plan, total, extra)
        if label == "dec_0":
            latest_gate, latest_up = kept
        if label == "dec_1":
            column_gate, column_up = kept
        if label == "dec_3":
            (serve_norm,) = kept
    return (outs[0], outs[1], column_gate, column_up, serve_norm, latest_gate, latest_up)


def solution(mesh):
    torus = Mesh(mesh.devices.reshape(4, 4, 2, mesh.shape["cols"]), ALL)
    whole = P(ROWS, "x")
    return jax.shard_map(
        local,
        mesh=torus,
        in_specs=(whole,) * 6 + (P(ALL),) * 2,
        out_specs=(P(None, "x"), P(None, "x"), P("x"), P("x"), P(), whole, whole),
        check_vma=False,
    )
```
